32 devices in a mesh: dom: 8 (over y, x, core), feat: 4 (over z).
Axes of the slice: x: 2, y: 2, z: 4, core: 2. Of those that a mesh axis runs over, the one named last changes fastest.
Arguments:
- features: bfloat16 [128, 131072], P('feat', 'dom'), may hold values from -6 to 6
- seed_rows: int32 [2048], P('dom'), may hold values from 0 to 16383
- want_rows: int32 [8, 8, 128], P('dom'), may hold values from 0 to 16383
- live_counts: int32 [8, 8], P('dom'), may hold values from 1 to 128, as said below
- hop_one: int32 [15, 2048], P(None, 'dom'), may hold values from 0 to 1023, as said below
- hop_two: int32 [10, 15, 2048], P(None, None, 'dom'), may hold values from 0 to 1023, as said below
- w1_self: bfloat16 [256, 128], replicated, may hold values from -0.5 to 0.5
- w1_neigh: bfloat16 [256, 128], replicated, may hold values from -0.5 to 0.5
- b1: float32 [256], P('feat'), may hold values from -4 to 4
- w2_self: bfloat16 [256, 256], P(None, 'feat'), may hold values from -0.375 to 0.375
- w2_neigh: bfloat16 [256, 256], P(None, 'feat'), may hold values from -0.375 to 0.375
- b2: float32 [256], P('feat'), may hold values from -4 to 4
Outputs:
- embed: float32 [256, 2048], P('feat', 'dom')
The draws below stay inside these ranges and needn't reach their ends.
Inputs may be any that keep to these rules, and one draw needn't show every extreme that they name: `want_rows`: slots at or beyond live_counts[r, o] are ignored. `live_counts`: in every draw a quarter of the owners, every fourth one from a drawn offset, receive all 128 slots from every requester. `hop_one`: each entry is o * 128 + c, a position in the buffer of the requester that holds seed s, with c < live_counts of that requester and owner o. `hop_two`: each entry is o * 128 + c, a position in the buffer of the requester that holds seed s, with c < live_counts of that requester and owner o.
All inputs are finite; a program needn't handle non-finite values.
Results may differ from the reference program's by a relative error of at most 0.00036.
Values may be sent and summed in bfloat16 or wider, within the bound.
No kernel may reach another device: no remote copies, remote signals or barrier semaphores. Data moves between devices by JAX's collectives and lax.ppermute only.
A program may use at most 64 MiB of HBM per device.

```python
import jax
import jax.numpy as jnp
from jax import lax

FEAT = 128
HID = 256
OUT = 256
FAN1 = 15
FAN2 = 10
CAP = 128
SEED_DEV = 256
NODE_DEV = 16384
OWNERS = 8
SEEDS = 2048
NODES = 131072


def slot_plan(key):
    offset = jax.random.randint(jax.random.fold_in(key, 501), (), 0, 4)
    owner = jnp.arange(OWNERS, dtype=jnp.int32)
    spread = jax.random.randint(jax.random.fold_in(key, 502), (OWNERS, OWNERS), CAP // 8, CAP + 1)
    full = ((owner - offset) % 4 == 0)[None, :]
    return (offset, jnp.where(full, CAP, spread).astype(jnp.int32))


def positions(key, salt, lead):
    offset, counts = slot_plan(key)
    draw_key = jax.random.fold_in(key, salt)
    shape = lead + (SEEDS,)
    requester = jnp.broadcast_to(jnp.arange(SEEDS, dtype=jnp.int32) // SEED_DEV, shape)
    choose = jax.random.randint(jax.random.fold_in(draw_key, 1), shape, 0, 2)
    favored = (offset + 4 * jax.random.randint(jax.random.fold_in(draw_key, 2), shape, 0, OWNERS // 4)) % OWNERS
    anyone = jax.random.randint(jax.random.fold_in(draw_key, 3), shape, 0, OWNERS)
    owner = jnp.where(choose == 1, favored, anyone).astype(jnp.int32)
    limit = counts[requester, owner]
    slot = jax.random.randint(jax.random.fold_in(draw_key, 4), shape, 0, 1 << 20) % limit
    return (owner * CAP + slot).astype(jnp.int32)


def draw_live_counts(key, part):
    return slot_plan(key)[1]


def draw_hop_one(key, part):
    return positions(key, 11, (FAN1,))


def draw_hop_two(key, part):
    return positions(key, 12, (FAN2, FAN1))


def plant(values, stream_key, least, top_value):
    spot = [jax.random.randint(jax.random.fold_in(stream_key, axis), (), 0, length) for axis, length in enumerate(values.shape)]
    widest = values.shape.index(max(values.shape))
    neighbour = spot[:widest] + [(spot[widest] + 1) % values.shape[widest]] + spot[widest + 1:]
    return values.at[tuple(spot)].set(least).at[tuple(neighbour)].set(top_value)


def block_levels(rng, dims, cuts, least, top_value):
    gain = 1.0
    for axis_at, blocks in cuts:
        steps = jax.random.uniform(jax.random.fold_in(jax.random.fold_in(rng, 6), axis_at), (blocks,), jnp.float32, least / len(cuts), top_value / len(cuts))
        gain = gain * jnp.repeat(jnp.exp(steps), dims[axis_at] // blocks).reshape((-1,) + (1,) * (len(dims) - 1 - axis_at))
    return gain


def centred(own_key, dims, scale, most, pieces=(), kind=jnp.bfloat16):
    level = block_levels(own_key, dims, pieces, -0.22, 0.18) if pieces else 1.0
    entries = jax.random.normal(own_key, dims, jnp.float32) * scale * level
    return jnp.minimum(jnp.maximum(entries, -most), most).astype(kind)


def setup_inputs(seed: int = 0) -> dict:
    arg_keys = jax.random.split(jax.random.key(seed), 13)
    features = centred(arg_keys[0], (FEAT, NODES), 1.0, 6.0, ((0, 4), (1, 8)))
    seed_rows = plant(jax.random.randint(arg_keys[1], (SEEDS,), 0, NODE_DEV), jax.random.fold_in(arg_keys[1], 1), 0, NODE_DEV - 1).astype(jnp.int32)
    want_rows = plant(jax.random.randint(arg_keys[2], (OWNERS, OWNERS, CAP), 0, NODE_DEV), jax.random.fold_in(arg_keys[2], 1), 0, NODE_DEV - 1).astype(jnp.int32)
    live_counts = draw_live_counts(jax.random.fold_in(arg_keys[12], 71), 0)
    hop_one = draw_hop_one(jax.random.fold_in(arg_keys[12], 71), 0)
    hop_two = draw_hop_two(jax.random.fold_in(arg_keys[12], 71), 0)
    w1_self = centred(arg_keys[6], (HID, FEAT), FEAT ** -0.5, 0.5)
    w1_neigh = centred(arg_keys[7], (HID, FEAT), FEAT ** -0.5, 0.5)
    b1 = centred(arg_keys[8], (HID,), 1.0, 4.0, ((0, 4),), jnp.float32)
    w2_self = centred(arg_keys[9], (OUT, HID), HID ** -0.5, 0.375, ((1, 4),))
    w2_neigh = centred(arg_keys[10], (OUT, HID), HID ** -0.5, 0.375, ((1, 4),))
    b2 = centred(arg_keys[11], (OUT,), 1.0, 4.0, ((0, 4),), jnp.float32)
    return {"features": features, "seed_rows": seed_rows, "want_rows": want_rows, "live_counts": live_counts, "hop_one": hop_one, "hop_two": hop_two, "w1_self": w1_self, "w1_neigh": w1_neigh, "b1": b1, "w2_self": w2_self, "w2_neigh": w2_neigh, "b2": b2}


def reference(features, seed_rows, want_rows, live_counts, hop_one, hop_two, w1_self, w1_neigh, b1, w2_self, w2_neigh, b2):
    owner = jnp.arange(OWNERS, dtype=jnp.int32)
    nodes = want_rows + (owner * NODE_DEV)[None, :, None]
    fetched = jnp.take(features, nodes.reshape(-1).astype(jnp.int32), axis=1)
    slot = jnp.arange(CAP, dtype=jnp.int32)
    live = slot[None, None, :] < live_counts[:, :, None]
    fetched = jnp.where(live.reshape(1, -1), fetched, jnp.zeros((), fetched.dtype))
    requester = jnp.arange(SEEDS, dtype=jnp.int32) // SEED_DEV
    base = requester * (OWNERS * CAP)
    x_one = jnp.take(fetched, (hop_one + base[None, :]).reshape(-1).astype(jnp.int32), axis=1)

    def add_hop(number, total):
        picked = jnp.take(fetched, (hop_two[number] + base[None, :]).reshape(-1).astype(jnp.int32), axis=1)
        return total + picked.astype(jnp.float32)
    m_two = lax.fori_loop(0, FAN2, add_hop, jnp.zeros((FEAT, FAN1 * SEEDS), jnp.float32))
    m_two = (m_two * (1.0 / FAN2)).astype(jnp.bfloat16)
    x_seed = jnp.take(features, (seed_rows + requester * NODE_DEV).astype(jnp.int32), axis=1)
    m_one = (lax.optimization_barrier(jnp.sum(x_one.reshape(FEAT, FAN1, SEEDS).astype(jnp.float32), axis=1)) * (1.0 / FAN1)).astype(jnp.bfloat16)

    def layer(selves, means):
        pre = jnp.dot(w1_self, selves, preferred_element_type=jnp.float32)
        pre = pre + jnp.dot(w1_neigh, means, preferred_element_type=jnp.float32) + b1[:, None]
        return jnp.maximum(pre, 0.0)
    h_one = layer(x_one, m_two)
    h_seed = layer(x_seed, m_one)
    g_mean = lax.optimization_barrier(jnp.sum(h_one.reshape(HID, FAN1, SEEDS), axis=1)) * (1.0 / FAN1)
    z_out = jnp.dot(w2_self.astype(jnp.float32), h_seed, precision=lax.Precision.HIGHEST, preferred_element_type=jnp.float32)
    z_out = z_out + jnp.dot(w2_neigh.astype(jnp.float32), g_mean, precision=lax.Precision.HIGHEST, preferred_element_type=jnp.float32) + b2[:, None]
    square = lax.optimization_barrier(jnp.sum(z_out * z_out, axis=0))
    return z_out * lax.rsqrt(square * (1.0 / OUT) + 1.0)
```

```python
import functools

import jax
import jax.numpy as jnp
from jax import lax
from jax.experimental import pallas as pl
from jax.experimental.pallas import tpu as pltpu
from jax.sharding import PartitionSpec as P

BF16 = jnp.bfloat16
F32 = jnp.float32
LANES = 256
PARTS = 3


def pick_columns(feats_ref, rows, emit):
    feat_dev, nodes = feats_ref.shape
    group = max(1, min(256 // feat_dev, nodes // LANES))
    for start in range(0, rows.shape[1], LANES):
        want = rows[:, start : start + LANES]
        width = want.shape[1]
        high = want >> 8
        low = want & (LANES - 1)
        place = lax.broadcasted_iota(jnp.int32, (LANES, width), 0)
        pick = jnp.where(low == place, 1.0, 0.0).astype(BF16)
        total = jnp.zeros((feat_dev, width), F32)
        for first in range(0, nodes // LANES, group):
            left = jnp.concatenate(
                [
                    feats_ref[:, (first + i) * LANES : (first + i + 1) * LANES]
                    for i in range(group)
                ],
                axis=0,
            )
            part = jnp.dot(left, pick, preferred_element_type=F32)
            for i in range(group):
                total = jnp.where(
                    high == first + i, part[i * feat_dev : (i + 1) * feat_dev], total
                )
        emit(start, total)


def seed_kernel(feats_ref, rows_ref, w2s_ref, w2n_ref, bias_ref, out_ref):
    outs, hid_dev = w2s_ref.shape
    feat_dev = feats_ref.shape[0]
    out_ref[0:outs, 0:hid_dev] = w2s_ref[...]
    out_ref[0:outs, hid_dev : 2 * hid_dev] = w2n_ref[...]

    def emit(start, value):
        halves = value.shape[1] // 128
        for i in range(halves):
            at = outs + (start // 128 + i) * feat_dev
            out_ref[at : at + feat_dev, :] = value[:, i * 128 : (i + 1) * 128].astype(BF16)

    pick_columns(feats_ref, rows_ref[...], emit)
    rest = bias_ref[...]
    base = outs + (rows_ref.shape[1] // 128) * feat_dev
    for i in range(PARTS):
        piece = rest.astype(BF16)
        rest = rest - piece.astype(F32)
        out_ref[base + 16 * i : base + 16 * (i + 1), :] = jnp.broadcast_to(piece, (16, 128))


def fetch_kernel(feat, feats_ref, rows_ref, out_ref):
    def emit(start, value):
        for i in range(value.shape[1] // 128):
            piece = value[:, i * 128 : (i + 1) * 128].astype(BF16)
            for copy in range(feat):
                out_ref[(start // 128 + i) * feat + copy] = piece

    pick_columns(feats_ref, rows_ref[...], emit)


def layer_kernel(
    feat,
    live_ref,
    fetched_ref,
    one_ref,
    two_ref,
    w1s_ref,
    w1n_ref,
    *rest,
):
    pieces = rest[:feat]
    out_ref, table, times, w1, bias_out, x_seed, x_sum, g_sum = rest[feat:]
    owners, feats, cap = fetched_ref.shape
    fan_one, seeds = one_ref.shape
    fan_two = two_ref.shape[0]
    hidden = w1s_ref.shape[0]
    hid_dev = hidden // feat
    feat_dev = feats // feat
    outs = hidden
    me = lax.axis_index("feat")

    slot = lax.broadcasted_iota(jnp.int32, (feats, cap), 1)
    for owner in range(owners):
        value = fetched_ref[owner].astype(F32)
        value = jnp.where(slot < live_ref[0, owner], value, 0.0)
        table[owner // 2, :, (owner % 2) * cap : (owner % 2 + 1) * cap] = value.astype(BF16)

    for sample in range(fan_two):
        total = jnp.zeros((fan_one, seeds), F32)
        for other in range(fan_two):
            total = total + jnp.where(two_ref[sample] == two_ref[other], 1.0, 0.0)
        times[sample] = total

    bias_base = outs + (seeds // 128) * feat_dev
    bias_one = []
    for k in range(feat):
        owner = lax.rem(me - k + feat, feat)
        rows = pl.ds(pl.multiple_of(owner * hid_dev, hid_dev), hid_dev)
        w1[k * hid_dev : (k + 1) * hid_dev, 0:feats] = w1s_ref[rows, :]
        w1[k * hid_dev : (k + 1) * hid_dev, feats : 2 * feats] = w1n_ref[rows, :]
        at = pl.multiple_of(owner * feat_dev, feat_dev)
        for i in range(seeds // 128):
            first = outs + i * feat_dev
            x_seed[pl.ds(at, feat_dev), i * 128 : (i + 1) * 128] = pieces[k][
                first : first + feat_dev, 0:128
            ]
        bias = jnp.zeros((8, 128), F32)
        for i in range(PARTS):
            bias = bias + pieces[k][bias_base + 16 * i : bias_base + 16 * (i + 1), :][0:8].astype(F32)
        column = bias.T
        bias_one.append(column[0:hid_dev, 0:1])
        bias_out[rows, :] = jnp.broadcast_to(column[hid_dev : 2 * hid_dev, 0:1], (hid_dev, 128))
    bias_one = jnp.concatenate(bias_one, axis=0)

    x_sum[...] = jnp.zeros_like(x_sum)
    g_sum[...] = jnp.zeros_like(g_sum)
    blocks = table.shape[0]
    block = table.shape[2]
    place = lax.broadcasted_iota(jnp.int32, (block, seeds), 0).astype(F32).astype(BF16)

    def low_row(value, start):
        moved = value - start
        inside = (moved >= 0) & (moved < block)
        return jnp.where(inside, moved, -1).astype(F32).astype(BF16)

    def step(j, carry):
        first = one_ref[pl.ds(j, 1), :]
        second = [two_ref[k, pl.ds(j, 1), :] for k in range(fan_two)]
        weight = [times[k, pl.ds(j, 1), :].astype(BF16) for k in range(fan_two)]
        own = jnp.zeros((feats, seeds), F32)
        mean = jnp.zeros((feats, seeds), F32)
        one = jnp.ones((), BF16)
        zero = jnp.zeros((), BF16)
        for b in range(blocks):
            pick = jnp.where(low_row(first, b * block) == place, one, zero)
            own = own + jnp.dot(table[b], pick, preferred_element_type=F32)
            count = jnp.zeros((block, seeds), BF16)
            for k in range(fan_two):
                count = jnp.where(low_row(second[k], b * block) == place, weight[k], count)
            mean = mean + jnp.dot(table[b], count, preferred_element_type=F32)
        x_sum[...] += own
        both = jnp.concatenate(
            [own.astype(BF16), (mean * (1.0 / fan_two)).astype(BF16)], axis=0
        )
        pre = jnp.dot(w1[...], both, preferred_element_type=F32)
        g_sum[...] += jnp.maximum(pre + bias_one, 0.0)
        return carry

    lax.fori_loop(0, fan_one, step, 0)

    m_one = (x_sum[...] * (1.0 / fan_one)).astype(BF16)
    both = jnp.concatenate([x_seed[...], m_one], axis=0)
    h_seed = jnp.maximum(jnp.dot(w1[...], both, preferred_element_type=F32) + bias_one, 0.0)
    g_mean = g_sum[...] * (1.0 / fan_one)
    z = jnp.zeros((outs, seeds), F32) + bias_out[:, 0:1]
    for index, value in enumerate((h_seed, g_mean)):
        w2 = jnp.concatenate(
            [
                pieces[k][0:outs, :][:, index * hid_dev : (index + 1) * hid_dev]
                for k in range(feat)
            ],
            axis=1,
        )
        high = value.astype(BF16)
        low = (value - high.astype(F32)).astype(BF16)
        z = z + jnp.dot(w2, high, preferred_element_type=F32)
        z = z + jnp.dot(w2, low, preferred_element_type=F32)
    square = jnp.sum(z * z, axis=0, keepdims=True)
    z = z * lax.rsqrt(square * (1.0 / outs) + 1.0)
    out_dev = out_ref.shape[0]
    x_sum_full = g_sum
    x_sum_full[...] = z
    out_ref[...] = x_sum_full[pl.ds(pl.multiple_of(me * out_dev, out_dev), out_dev), :]


def per_device(
    features,
    seed_rows,
    want_rows,
    live_counts,
    hop_one,
    hop_two,
    w1_self,
    w1_neigh,
    b1,
    w2_self,
    w2_neigh,
    b2,
):
    feat_dev = features.shape[0]
    seed_dev = seed_rows.shape[0]
    hid_dev = b1.shape[0]
    owners, cap = want_rows.shape[1:]
    feat = lax.axis_size("feat")
    feats = feat * feat_dev
    outs, hidden = w1_self.shape[0], w1_self.shape[0]
    vmem = pl.BlockSpec(memory_space=pltpu.VMEM)
    smem = pl.BlockSpec(memory_space=pltpu.SMEM)

    asked = lax.all_to_all(want_rows, "dom", split_axis=1, concat_axis=0, tiled=True)
    bias = jnp.concatenate([b1, b2, jnp.zeros((128 - 2 * hid_dev,), F32)])[None]
    rows = outs + (seed_dev // 128) * feat_dev + 16 * PARTS
    mine = pl.pallas_call(
        seed_kernel,
        out_shape=jax.ShapeDtypeStruct((rows, 128), BF16),
        in_specs=[vmem] * 5,
        out_specs=vmem,
        name="seed_kernel",
    )(features, seed_rows[None], w2_self, w2_neigh, bias)
    pieces = [mine] + [
        lax.ppermute(mine, "feat", [(i, (i + k) % feat) for i in range(feat)])
        for k in range(1, feat)
    ]
    served = pl.pallas_call(
        functools.partial(fetch_kernel, feat),
        out_shape=jax.ShapeDtypeStruct((owners * feat, feat_dev, cap), BF16),
        in_specs=[vmem] * 2,
        out_specs=vmem,
        name="fetch_kernel",
    )(features, asked.reshape(1, owners * cap))
    fetched = lax.all_to_all(served, ("dom", "feat"), split_axis=0, concat_axis=0, tiled=True)
    fetched = fetched.reshape(owners, feats, cap)
    return pl.pallas_call(
        functools.partial(layer_kernel, feat),
        out_shape=jax.ShapeDtypeStruct((outs // feat, seed_dev), F32),
        in_specs=[smem] + [vmem] * (5 + feat),
        out_specs=vmem,
        scratch_shapes=[
            pltpu.VMEM((owners // 2, feats, 2 * cap), BF16),
            pltpu.VMEM(hop_two.shape, F32),
            pltpu.VMEM((hidden, 2 * feats), BF16),
            pltpu.VMEM((outs, 128), F32),
            pltpu.VMEM((feats, seed_dev), BF16),
            pltpu.VMEM((feats, seed_dev), F32),
            pltpu.VMEM((outs, seed_dev), F32),
        ],
        name="layer_kernel",
    )(live_counts, fetched, hop_one, hop_two, w1_self, w1_neigh, *pieces)


def solution(mesh):
    return jax.shard_map(
        per_device,
        mesh=mesh,
        in_specs=(
            P("feat", "dom"),
            P("dom"),
            P("dom", None, None),
            P("dom", None),
            P(None, "dom"),
            P(None, None, "dom"),
            P(),
            P(),
            P("feat"),
            P(None, "feat"),
            P(None, "feat"),
            P("feat"),
        ),
        out_specs=P("feat", "dom"),
        check_vma=False,
    )
```

```python
import functools

import jax
import jax.numpy as jnp
from jax import lax
from jax.experimental import pallas as pl
from jax.experimental.pallas import tpu as pltpu
from jax.sharding import PartitionSpec as P


BF16 = jnp.bfloat16
F32 = jnp.float32
LANES = 256
PARTS = 3
STAGED_BYTES = 1 << 23
TILE = 16
GROUP = 3
COUNT = jnp.float8_e4m3fn


def from_where(me, k, feat):
    if feat & (feat - 1) == 0:
        return me ^ k
    return (me - k) % feat


def in_hbm(x):
    return pltpu.with_memory_space_constraint(x, pltpu.HBM)


def grant(mib, flops):
    return dict(
        compiler_params=pltpu.CompilerParams(vmem_limit_bytes=mib << 20),
        cost_estimate=pl.CostEstimate(flops=flops, bytes_accessed=1 << 20, transcendentals=0),
    )


def pick_columns(feats_ref, rows, emit):
    feat_dev, nodes = feats_ref.shape
    group = max(1, min(256 // feat_dev, nodes // LANES))
    for start in range(0, rows.shape[1], LANES):
        want = rows[:, start : start + LANES]
        width = want.shape[1]
        high = want >> 8
        low = want & (LANES - 1)
        place = lax.broadcasted_iota(jnp.int32, (LANES, width), 0)
        pick = jnp.where(low == place, 1.0, 0.0).astype(BF16)
        total = jnp.zeros((feat_dev, width), F32)
        for first in range(0, nodes // LANES, group):
            left = jnp.concatenate(
                [
                    feats_ref[:, (first + i) * LANES : (first + i + 1) * LANES]
                    for i in range(group)
                ],
                axis=0,
            )
            part = jnp.dot(left, pick, preferred_element_type=F32)
            for i in range(group):
                total = jnp.where(
                    high == first + i, part[i * feat_dev : (i + 1) * feat_dev], total
                )
        emit(start, total)


def seed_kernel(feats_ref, rows_ref, w2s_ref, w2n_ref, b1_ref, b2_ref, out_ref, near_ref):
    hid_dev, outs = w2s_ref.shape
    feat_dev = feats_ref.shape[0]
    out_ref[0:outs, 0:hid_dev] = w2s_ref[...].astype(F32).T.astype(BF16)
    out_ref[0:outs, hid_dev : 2 * hid_dev] = w2n_ref[...].astype(F32).T.astype(BF16)

    def emit(start, value):
        for i in range(value.shape[1] // 128):
            at = outs + (start // 128 + i) * feat_dev
            out_ref[at : at + feat_dev, :] = value[:, i * 128 : (i + 1) * 128].astype(BF16)

    pick_columns(feats_ref, rows_ref[...], emit)
    near_ref[...] = feats_ref[...]
    base = outs + (rows_ref.shape[1] // 128) * feat_dev
    for at, bias_ref in ((0, b1_ref), (hid_dev, b2_ref)):
        rest = jnp.broadcast_to(bias_ref[...], (16, hid_dev))
        line = lax.broadcasted_iota(jnp.int32, rest.shape, 0)
        parts = jnp.zeros_like(rest)
        for i in range(PARTS):
            piece = rest.astype(BF16).astype(F32)
            rest = rest - piece
            parts = jnp.where(line == i, piece, parts)
        out_ref[base : base + 16, at : at + hid_dev] = parts.astype(BF16)


def fetch_kernel(feat, feats_ref, rows_ref, out_ref):
    def emit(start, value):
        for i in range(value.shape[1] // 128):
            piece = value[:, i * 128 : (i + 1) * 128].astype(BF16)
            for copy in range(feat):
                out_ref[(start // 128 + i) * feat + copy] = piece

    pick_columns(feats_ref, rows_ref[...], emit)


def multiplicities(two_ref, times):
    fan_two, fan_one, seeds = two_ref.shape
    for sample in range(fan_two):
        total = jnp.zeros((fan_one, seeds), F32)
        for other in range(fan_two):
            total = total + jnp.where(two_ref[sample] == two_ref[other], 1.0, 0.0)
        times[sample] = total


def block_picks(first, second, weight, start, block):
    seeds = first.shape[1]
    place = lax.broadcasted_iota(jnp.int32, (block, seeds), 0).astype(F32).astype(BF16)

    def low_row(value):
        moved = value - start
        inside = (moved >= 0) & (moved < block)
        return jnp.where(inside, moved, -1).astype(F32).astype(BF16)

    one = jnp.ones((), BF16)
    zero = jnp.zeros((), BF16)
    pick = jnp.where(low_row(first) == place, one, zero)
    count = jnp.zeros((block, seeds), BF16)
    for value, times in zip(second, weight):
        count = jnp.where(low_row(value) == place, times, count)
    return pick, count


def pick_kernel(one_ref, two_ref, out_ref, times, made, sems):
    fan_one, seeds = one_ref.shape
    fan_two = two_ref.shape[0]
    slots = out_ref.shape[1]
    multiplicities(two_ref, times)
    line = lax.broadcasted_iota(jnp.int32, (TILE, 128), 0)
    zero = jnp.zeros((TILE, 128), BF16)
    one = jnp.ones((TILE, 128), BF16)

    def copy_of(j):
        return pltpu.make_async_copy(made.at[j], out_ref.at[j], sems.at[j])

    def step(j, carry):
        rows = [two_ref[k, pl.ds(j, 1), :] for k in range(fan_two)] + [one_ref[pl.ds(j, 1), :]]
        weights = [times[k, pl.ds(j, 1), :] for k in range(fan_two)]
        for at in range(0, seeds, 128):
            value = [
                jnp.broadcast_to(row[:, at : at + 128], (TILE, 128)).astype(jnp.int16)
                for row in rows
            ]
            times_of = [
                jnp.broadcast_to(row[:, at : at + 128], (TILE, 128)).astype(BF16)
                for row in weights
            ]
            for start in range(0, slots, 2 * TILE):
                first, second = [], []
                for half in (start, start + TILE):
                    place = (line + half).astype(jnp.int16)
                    count = zero
                    for k in range(fan_two):
                        count = jnp.where(value[k] == place, times_of[k], count)
                    first.append(jnp.where(value[fan_two] == place, one, zero))
                    second.append(count)
                for base, parts in ((0, first), (seeds, second)):
                    made[j, start : start + 2 * TILE, base + at : base + at + 128] = (
                        jnp.concatenate(parts, axis=0).astype(COUNT)
                    )
        copy_of(j).start()
        return carry

    lax.fori_loop(0, fan_one, step, 0)
    for j in range(fan_one):
        copy_of(j).wait()


def layer_kernel(feat, staged, fan_two, live_ref, fetched_ref, w1s_ref, w1n_ref, *rest):
    pieces = rest[:feat]
    picks = rest[feat : feat + (1 if staged else 2)]
    out_ref, table, staging, sems, w1, both, bias_out, x_seed, x_sum, g_sum = rest[feat + len(picks) :]
    owners, feats, cap = fetched_ref.shape
    fan_one = picks[0].shape[0]
    seeds = x_seed.shape[1]
    hidden = w1s_ref.shape[0]
    hid_dev = hidden // feat
    feat_dev = feats // feat
    outs = hidden
    me = lax.axis_index("feat")

    def copy_of(j):
        return pltpu.make_async_copy(picks[0].at[j], staging.at[j], sems.at[j])

    if staged:
        for j in range(fan_one):
            copy_of(j).start()
    slot = lax.broadcasted_iota(jnp.int32, (feats, cap), 1)
    for owner in range(owners):
        value = fetched_ref[owner].astype(F32)
        value = jnp.where(slot < live_ref[0, owner], value, 0.0)
        table[:, owner * cap : (owner + 1) * cap] = value.astype(BF16)
    if not staged:
        multiplicities(picks[1], staging)

    bias_base = outs + (seeds // 128) * feat_dev
    bias_one = []
    for k in range(feat):
        owner = from_where(me, k, feat)
        rows = pl.ds(pl.multiple_of(owner * hid_dev, hid_dev), hid_dev)
        w1[k * hid_dev : (k + 1) * hid_dev, 0:feats] = w1s_ref[rows, :]
        w1[k * hid_dev : (k + 1) * hid_dev, feats : 2 * feats] = w1n_ref[rows, :]
        at = pl.multiple_of(owner * feat_dev, feat_dev)
        for i in range(seeds // 128):
            first = outs + i * feat_dev
            x_seed[pl.ds(at, feat_dev), i * 128 : (i + 1) * 128] = pieces[k][
                first : first + feat_dev, 0:128
            ]
        parts = pieces[k][bias_base : bias_base + 16, :].astype(F32)
        bias = parts[0:1] + parts[1:2] + parts[2:3]
        column = jnp.broadcast_to(bias, (8, 128)).T
        bias_one.append(column[0:hid_dev, 0:1])
        bias_out[rows, :] = jnp.broadcast_to(column[hid_dev : 2 * hid_dev, 0:1], (hid_dev, 128))
    bias_one = jnp.concatenate(bias_one, axis=0)

    x_sum[...] = jnp.zeros_like(x_sum)

    def aggregate(j):
        if staged:
            copy_of(j).wait()
            sums = jnp.dot(table[...], staging[j], preferred_element_type=F32)
            return sums[:, 0:seeds], sums[:, seeds : 2 * seeds]
        one_ref, two_ref = picks
        first = one_ref[pl.ds(j, 1), :]
        second = [two_ref[k, pl.ds(j, 1), :] for k in range(fan_two)]
        weight = [staging[k, pl.ds(j, 1), :].astype(BF16) for k in range(fan_two)]
        own = jnp.zeros((feats, seeds), F32)
        mean = jnp.zeros((feats, seeds), F32)
        for start in range(0, owners * cap, LANES):
            pick, count = block_picks(first, second, weight, start, LANES)
            left = table[:, start : start + LANES]
            own = own + jnp.dot(left, pick, preferred_element_type=F32)
            mean = mean + jnp.dot(left, count, preferred_element_type=F32)
        return own, mean

    def step(j, carry):
        own, mean = aggregate(j)
        x_sum[...] += own
        both[j, 0:feats] = own.astype(BF16)
        both[j, feats : 2 * feats] = (mean * (1.0 / fan_two)).astype(BF16)
        return carry

    lax.fori_loop(0, fan_one, step, 0, unroll=3 if staged else 1)
    both[fan_one, 0:feats] = x_seed[...]
    both[fan_one, feats : 2 * feats] = (x_sum[...] * (1.0 / fan_one)).astype(BF16)

    g_sum[...] = jnp.zeros_like(g_sum)

    def layer(j):
        pre = jnp.dot(w1[...], both[j], preferred_element_type=F32)
        return jnp.maximum(pre + bias_one, 0.0)

    def add_layer(i, carry):
        total = layer(i * GROUP)
        for j in range(1, GROUP):
            total = total + layer(i * GROUP + j)
        g_sum[...] += total
        return carry

    lax.fori_loop(0, fan_one // GROUP, add_layer, 0)
    for j in range(fan_one // GROUP * GROUP, fan_one):
        g_sum[...] += layer(j)

    h_seed = layer(fan_one)
    g_mean = g_sum[...] * (1.0 / fan_one)
    z = jnp.zeros((outs, seeds), F32) + bias_out[:, 0:1]
    for index, value in enumerate((h_seed, g_mean)):
        w2 = jnp.concatenate(
            [
                pieces[k][0:outs, :][:, index * hid_dev : (index + 1) * hid_dev]
                for k in range(feat)
            ],
            axis=1,
        )
        high = value.astype(BF16)
        low = (value - high.astype(F32)).astype(BF16)
        z = z + jnp.dot(w2, high, preferred_element_type=F32)
        z = z + jnp.dot(w2, low, preferred_element_type=F32)
    square = jnp.sum(z * z, axis=0, keepdims=True)
    out_dev = out_ref.shape[0]
    g_sum[...] = z * lax.rsqrt(square * (1.0 / outs) + 1.0)
    out_ref[...] = g_sum[pl.ds(pl.multiple_of(me * out_dev, out_dev), out_dev), :]


def per_device(
    features,
    seed_rows,
    want_rows,
    live_counts,
    hop_one,
    hop_two,
    w1_self,
    w1_neigh,
    b1,
    w2_self,
    w2_neigh,
    b2,
):
    feat_dev = features.shape[0]
    seed_dev = seed_rows.shape[0]
    owners, cap = want_rows.shape[1:]
    feat = lax.axis_size("feat")
    feats = feat * feat_dev
    outs, hidden = w1_self.shape[0], w1_self.shape[0]
    slots = owners * cap
    fan_two, fan_one = hop_two.shape[:2]
    staged = fan_one * slots * 2 * seed_dev <= STAGED_BYTES
    vmem = pl.BlockSpec(memory_space=pltpu.VMEM)
    hbm = pl.BlockSpec(memory_space=pltpu.HBM)
    smem = pl.BlockSpec(memory_space=pltpu.SMEM)

    asked = lax.all_to_all(want_rows, "dom", split_axis=1, concat_axis=0, tiled=True)
    rows = outs + (seed_dev // 128) * feat_dev + 16
    mine, near = pl.pallas_call(
        seed_kernel,
        out_shape=[
            jax.ShapeDtypeStruct((rows, 128), BF16),
            jax.ShapeDtypeStruct(features.shape, BF16),
        ],
        in_specs=[vmem] * 6,
        out_specs=[vmem] * 2,
        name="seed_kernel",
        **grant(8, 10**9),
    )(features, *map(in_hbm, (seed_rows[None], w2_self.T, w2_neigh.T, b1[None], b2[None])))
    pieces = [mine]
    for k in range(1, feat):
        pairs = [(from_where(i, k, feat), i) for i in range(feat)]
        pieces.append(lax.ppermute(mine, "feat", pairs))
    fetch = pl.pallas_call(
        functools.partial(fetch_kernel, feat),
        out_shape=jax.ShapeDtypeStruct((owners * feat, feat_dev, cap), BF16),
        in_specs=[vmem] * 2,
        out_specs=vmem,
        name="fetch_kernel",
        **grant(8, 10**9),
    )
    served = fetch(near, asked.reshape(1, slots))
    fetched = lax.all_to_all(
        served, ("dom", "feat"), split_axis=0, concat_axis=0, tiled=True
    )
    fetched = fetched.reshape(owners, feats, cap)
    picks = (hop_one, hop_two)
    staging = pltpu.VMEM(hop_two.shape, F32)
    if staged:
        picks = (
            pl.pallas_call(
                pick_kernel,
                out_shape=pltpu.HBM((fan_one, slots, 2 * seed_dev), COUNT),
                in_specs=[vmem] * 2,
                out_specs=hbm,
                scratch_shapes=[
                    pltpu.VMEM(hop_two.shape, F32),
                    pltpu.VMEM((fan_one, slots, 2 * seed_dev), COUNT),
                    pltpu.SemaphoreType.DMA((fan_one,)),
                ],
                name="pick_kernel",
                **grant(12, 5 * 10**9),
            )(in_hbm(hop_one), in_hbm(hop_two)),
        )
        staging = pltpu.VMEM(picks[0].shape, COUNT)
    return pl.pallas_call(
        functools.partial(layer_kernel, feat, staged, fan_two),
        out_shape=jax.ShapeDtypeStruct((outs // feat, seed_dev), F32),
        in_specs=[smem] + [vmem] * (3 + feat) + [hbm if staged else vmem] * len(picks),
        out_specs=vmem,
        scratch_shapes=[
            pltpu.VMEM((feats, slots), BF16),
            staging,
            pltpu.SemaphoreType.DMA((fan_one,)),
            pltpu.VMEM((hidden, 2 * feats), BF16),
            pltpu.VMEM((fan_one + 1, 2 * feats, seed_dev), BF16),
            pltpu.VMEM((outs, 128), F32),
            pltpu.VMEM((feats, seed_dev), BF16),
            pltpu.VMEM((feats, seed_dev), F32),
            pltpu.VMEM((outs, seed_dev), F32),
        ],
        name="layer_kernel",
        **grant(24, 5 * 10**9),
    )(live_counts, fetched, w1_self, w1_neigh, *pieces, *(map(in_hbm, picks) if staged else picks))


def solution(mesh):
    return jax.shard_map(
        per_device,
        mesh=mesh,
        in_specs=(
            P("feat", "dom"),
            P("dom"),
            P("dom", None, None),
            P("dom", None),
            P(None, "dom"),
            P(None, None, "dom"),
            P(),
            P(),
            P("feat"),
            P(None, "feat"),
            P(None, "feat"),
            P("feat"),
        ),
        out_specs=P("feat", "dom"),
        check_vma=False,
    )
```

```python
import functools

import jax
import jax.numpy as jnp
from jax import lax
from jax.experimental import pallas as pl
from jax.experimental.pallas import tpu as pltpu
from jax.sharding import PartitionSpec as P


BF16 = jnp.bfloat16
F32 = jnp.float32
LANES = 256
PARTS = 3
HELD_BYTES = 1 << 21
TILE = 32
GROUP = 3
LOADS = 4
SMALLS = 5
COUNT = jnp.float8_e4m3fn


def from_where(me, k, feat):
    if feat & (feat - 1) == 0:
        return me ^ k
    return (me - k) % feat


def unroll_of(count):
    return next(u for u in (5, 4, 3, 2, 1) if count % u == 0)


def in_hbm(x):
    return pltpu.with_memory_space_constraint(x, pltpu.HBM)


def grant(mib, flops):
    return dict(
        compiler_params=pltpu.CompilerParams(vmem_limit_bytes=mib << 20),
        cost_estimate=pl.CostEstimate(flops=flops, bytes_accessed=1 << 20, transcendentals=0),
    )


def pick_columns(feats_ref, rows, emit, ready=None):
    feat_dev, nodes = feats_ref.shape
    group = max(1, min(256 // feat_dev, nodes // LANES))
    for start in range(0, rows.shape[1], LANES):
        want = rows[:, start : start + LANES]
        width = want.shape[1]
        high = want >> 8
        low = want & (LANES - 1)
        place = lax.broadcasted_iota(jnp.int32, (LANES, width), 0)
        pick = jnp.where(low == place, 1.0, 0.0).astype(BF16)
        total = jnp.zeros((feat_dev, width), F32)
        for first in range(0, nodes // LANES, group):
            if ready is not None and start == 0:
                ready(first * LANES)
            left = jnp.concatenate(
                [
                    feats_ref[:, (first + i) * LANES : (first + i + 1) * LANES]
                    for i in range(group)
                ],
                axis=0,
            )
            part = jnp.dot(left, pick, preferred_element_type=F32)
            for i in range(group):
                total = jnp.where(
                    high == first + i, part[i * feat_dev : (i + 1) * feat_dev], total
                )
        emit(start, total)


def early_kernel(feats_ref, *rest):
    sources, (out_ref, near_ref, sems), scratch = rest[:SMALLS], rest[SMALLS : SMALLS + 3], rest[-SMALLS:]
    rows_ref, w2s_ref, w2n_ref, b1_ref, b2_ref = scratch
    hid_dev, outs = w2s_ref.shape
    feat_dev, nodes = feats_ref.shape
    loads = LOADS
    width = nodes // loads
    smalls = [
        pltpu.make_async_copy(source, scratch[i], sems.at[loads + i])
        for i, source in enumerate(sources)
    ]

    def load(i):
        part = (slice(None), pl.ds(i * width, width))
        return pltpu.make_async_copy(feats_ref.at[part], near_ref.at[part], sems.at[i])

    for copy in smalls:
        copy.start()
    for i in range(loads):
        load(i).start()
    for copy in smalls:
        copy.wait()
    out_ref[0:outs, 0:hid_dev] = w2s_ref[...].astype(F32).T.astype(BF16)
    out_ref[0:outs, hid_dev : 2 * hid_dev] = w2n_ref[...].astype(F32).T.astype(BF16)
    base = outs + (rows_ref.shape[1] // 128) * feat_dev
    for at, bias_ref in ((0, b1_ref), (hid_dev, b2_ref)):
        left = jnp.broadcast_to(bias_ref[...], (16, hid_dev))
        line = lax.broadcasted_iota(jnp.int32, left.shape, 0)
        parts = jnp.zeros_like(left)
        for i in range(PARTS):
            piece = left.astype(BF16).astype(F32)
            left = left - piece
            parts = jnp.where(line == i, piece, parts)
        out_ref[base : base + 16, at : at + hid_dev] = parts.astype(BF16)

    def emit(start, value):
        for i in range(value.shape[1] // 128):
            at = outs + (start // 128 + i) * feat_dev
            out_ref[at : at + feat_dev, :] = value[:, i * 128 : (i + 1) * 128].astype(BF16)

    def ready(column):
        if column % width == 0:
            load(column // width).wait()

    pick_columns(near_ref, rows_ref[...], emit, ready)


def fetch_kernel(feat, feats_ref, rows_ref, out_ref):
    def emit(start, value):
        for i in range(value.shape[1] // 128):
            piece = value[:, i * 128 : (i + 1) * 128].astype(BF16)
            for copy in range(feat):
                out_ref[(start // 128 + i) * feat + copy] = piece

    pick_columns(feats_ref, rows_ref[...], emit)


def multiplicities(two_ref, times):
    fan_two, fan_one, seeds = two_ref.shape
    for sample in range(fan_two):
        total = jnp.zeros((fan_one, seeds), F32)
        for other in range(fan_two):
            total = total + jnp.where(two_ref[sample] == two_ref[other], 1.0, 0.0)
        times[sample] = total


def make_counts(first, count, two_ref, times, made, out_ref=None, sems=None):
    seeds = two_ref.shape[2]
    fan_two = two_ref.shape[0]
    slots = made.shape[1]
    shape = (TILE, 128)
    i8 = jnp.int8
    line = lax.broadcasted_iota(jnp.int32, shape, 0)
    places = [(line + TILE * i).astype(i8) for i in range(128 // TILE)]
    none = jnp.full(shape, -1, i8)

    def step(j, carry):
        at_j = pl.ds(first + j, 1)
        rows = [two_ref[k, at_j, :] for k in range(fan_two)]
        weights = [times[k, at_j, :] for k in range(fan_two)]
        for at in range(0, seeds, 128):
            wide = [jnp.broadcast_to(row[:, at : at + 128], shape) for row in rows]
            low = [(value & 127).astype(i8) for value in wide]
            high = [(value >> 7).astype(i8) for value in wide]
            times_of = [
                jnp.broadcast_to(row[:, at : at + 128], shape).astype(COUNT) for row in weights
            ]
            for block in range(slots // 128):
                here = jnp.full(shape, block, i8)
                value = [jnp.where(h == here, v, none) for h, v in zip(high, low)]
                for i, place in enumerate(places):
                    total = jnp.zeros(shape, COUNT)
                    for k in range(fan_two):
                        total = jnp.where(value[k] == place, times_of[k], total)
                    start = block * 128 + i * TILE
                    made[j, start : start + TILE, at : at + 128] = total
        if out_ref is not None:
            pltpu.make_async_copy(made.at[j], out_ref.at[j], sems.at[j]).start()
        return carry

    lax.fori_loop(0, count, step, 0)


def late_kernel(held, two_ref, held_ref, out_ref, times, made, sems):
    late = out_ref.shape[0]
    multiplicities(two_ref, times)
    make_counts(held, late, two_ref, times, made, out_ref, sems)
    make_counts(0, held, two_ref, times, held_ref)
    for j in range(late):
        pltpu.make_async_copy(made.at[j], out_ref.at[j], sems.at[j]).wait()


def prep_kernel(feat, w1s_ref, w1n_ref, *rest):
    pieces = rest[:feat]
    w1, w2, x_seed, bias_one, bias_out = rest[feat:]
    hidden, feats = w1s_ref.shape
    outs = w2.shape[1]
    hid_dev = hidden // feat
    feat_dev = feats // feat
    seeds = x_seed.shape[1]
    me = lax.axis_index("feat")
    bias_base = outs + (seeds // 128) * feat_dev
    for k in range(feat):
        owner = from_where(me, k, feat)
        rows = pl.ds(pl.multiple_of(owner * hid_dev, hid_dev), hid_dev)
        here = slice(k * hid_dev, (k + 1) * hid_dev)
        w1[here, 0:feats] = w1s_ref[rows, :]
        w1[here, feats : 2 * feats] = w1n_ref[rows, :]
        at = pl.multiple_of(owner * feat_dev, feat_dev)
        for i in range(seeds // 128):
            first = outs + i * feat_dev
            x_seed[pl.ds(at, feat_dev), i * 128 : (i + 1) * 128] = pieces[k][
                first : first + feat_dev, 0:128
            ]
        parts = pieces[k][bias_base : bias_base + 16, :].astype(F32)
        bias = parts[0:1] + parts[1:2] + parts[2:3]
        column = jnp.broadcast_to(bias, (8, 128)).T
        bias_one[here, :] = jnp.broadcast_to(column[0:hid_dev, 0:1], (hid_dev, 128))
        bias_out[rows, :] = jnp.broadcast_to(column[hid_dev : 2 * hid_dev, 0:1], (hid_dev, 128))
    for index in range(2):
        w2[index] = jnp.concatenate(
            [
                pieces[k][0:outs, :][:, index * hid_dev : (index + 1) * hid_dev]
                for k in range(feat)
            ],
            axis=1,
        )


def add_bias(value, bias_ref):
    return value + jnp.concatenate([bias_ref[...]] * (value.shape[1] // 128), axis=1)


def layer_kernel(
    fan_two, live_ref, fetched_ref, one_ref, w1, w2, x_seed, bias_one, bias_out, held_ref, late_ref, *rest
):
    out_ref, table, staging, sems, both, x_sum, g_sum = rest
    owners, feats, cap = fetched_ref.shape
    fan_one, seeds = one_ref.shape
    held, late = held_ref.shape[0], late_ref.shape[0]
    outs = w2.shape[1]
    me = lax.axis_index("feat")

    def late_copy(j):
        return pltpu.make_async_copy(late_ref.at[j], staging.at[j], sems.at[j])

    for j in range(late):
        late_copy(j).start()
    slot = lax.broadcasted_iota(jnp.int32, (feats, cap), 1)
    for owner in range(owners):
        value = fetched_ref[owner].astype(F32)
        value = jnp.where(slot < live_ref[0, owner], value, 0.0)
        table[:, owner * cap : (owner + 1) * cap] = value.astype(BF16)
    x_sum[...] = jnp.zeros_like(x_sum)

    def aggregate(j, counts):
        place = lax.broadcasted_iota(jnp.int32, (owners * cap, seeds), 0)
        pick = jnp.where(one_ref[pl.ds(j, 1), :] == place, 1.0, 0.0).astype(BF16)
        own = jnp.dot(table[...], pick, preferred_element_type=F32)
        mean = jnp.dot(table[...], counts, preferred_element_type=F32)
        x_sum[...] += own
        both[j, 0:feats] = own.astype(BF16)
        both[j, feats : 2 * feats] = (mean * (1.0 / fan_two)).astype(BF16)

    def held_step(j, carry):
        aggregate(j, held_ref[j])
        return carry

    def late_step(j, carry):
        late_copy(j).wait()
        aggregate(held + j, staging[j])
        return carry

    lax.fori_loop(0, held, held_step, 0, unroll=unroll_of(held))
    lax.fori_loop(0, late, late_step, 0, unroll=unroll_of(late))
    both[fan_one, 0:feats] = x_seed[...]
    both[fan_one, feats : 2 * feats] = (x_sum[...] * (1.0 / fan_one)).astype(BF16)

    g_sum[...] = jnp.zeros_like(g_sum)

    def layer(j):
        pre = jnp.dot(w1[...], both[j], preferred_element_type=F32)
        return jnp.maximum(add_bias(pre, bias_one), 0.0)

    def add_layer(i, carry):
        total = layer(i * GROUP)
        for j in range(1, GROUP):
            total = total + layer(i * GROUP + j)
        g_sum[...] += total
        return carry

    lax.fori_loop(0, fan_one // GROUP, add_layer, 0)
    for j in range(fan_one // GROUP * GROUP, fan_one):
        g_sum[...] += layer(j)

    z = add_bias(jnp.zeros((outs, seeds), F32), bias_out)
    for index, value in enumerate((layer(fan_one), g_sum[...] * (1.0 / fan_one))):
        high = value.astype(BF16)
        low = (value - high.astype(F32)).astype(BF16)
        z = z + jnp.dot(w2[index], high, preferred_element_type=F32)
        z = z + jnp.dot(w2[index], low, preferred_element_type=F32)
    square = jnp.sum(z * z, axis=0, keepdims=True)
    out_dev = out_ref.shape[0]
    g_sum[...] = z * lax.rsqrt(square * (1.0 / outs) + 1.0)
    out_ref[...] = g_sum[pl.ds(pl.multiple_of(me * out_dev, out_dev), out_dev), :]


def per_device(
    features,
    seed_rows,
    want_rows,
    live_counts,
    hop_one,
    hop_two,
    w1_self,
    w1_neigh,
    b1,
    w2_self,
    w2_neigh,
    b2,
):
    feat_dev = features.shape[0]
    seed_dev = seed_rows.shape[0]
    owners, cap = want_rows.shape[1:]
    feat = lax.axis_size("feat")
    feats = feat * feat_dev
    outs, hidden = w1_self.shape[0], w1_self.shape[0]
    slots = owners * cap
    fan_two, fan_one = hop_two.shape[:2]
    vmem = pl.BlockSpec(memory_space=pltpu.VMEM)
    hbm = pl.BlockSpec(memory_space=pltpu.HBM)
    smem = pl.BlockSpec(memory_space=pltpu.SMEM)

    asked = lax.all_to_all(want_rows, "dom", split_axis=1, concat_axis=0, tiled=True)
    rows = outs + (seed_dev // 128) * feat_dev + 16
    held = max(1, min(fan_one - 1, HELD_BYTES // (slots * seed_dev)))
    late = fan_one - held
    two_vmem = pltpu.VMEM(hop_two.shape, F32)
    smalls = (seed_rows[None], w2_self.T, w2_neigh.T, b1[None], b2[None])
    mine, near = pl.pallas_call(
        early_kernel,
        out_shape=[pltpu.VMEM((rows, 128), BF16), pltpu.VMEM(features.shape, BF16)],
        in_specs=[hbm] * (1 + SMALLS),
        out_specs=[vmem] * 2,
        scratch_shapes=[pltpu.SemaphoreType.DMA((LOADS + SMALLS,))]
        + [pltpu.VMEM(x.shape, x.dtype) for x in smalls],
        name="early_kernel",
        **grant(8, 10**9),
    )(*map(in_hbm, (features,) + smalls))
    pieces = [mine]
    for k in range(1, feat):
        pairs = [(from_where(i, k, feat), i) for i in range(feat)]
        pieces.append(lax.ppermute(mine, "feat", pairs))
    fetch = pl.pallas_call(
        functools.partial(fetch_kernel, feat),
        out_shape=pltpu.VMEM((owners * feat, feat_dev, cap), BF16),
        in_specs=[vmem] * 2,
        out_specs=vmem,
        name="fetch_kernel",
        **grant(8, 10**9),
    )
    served = fetch(near, asked.reshape(1, slots))
    fetched = lax.all_to_all(
        served, ("dom", "feat"), split_axis=0, concat_axis=0, tiled=True
    )
    fetched = fetched.reshape(owners, feats, cap)
    block = (slots, seed_dev)
    staging = pltpu.VMEM((late,) + block, COUNT)
    held_counts, late_counts = pl.pallas_call(
        functools.partial(late_kernel, held),
        out_shape=[pltpu.VMEM((held,) + block, COUNT), pltpu.HBM((late,) + block, COUNT)],
        in_specs=[vmem],
        out_specs=[vmem, hbm],
        scratch_shapes=[two_vmem, staging, pltpu.SemaphoreType.DMA((late,))],
        name="late_kernel",
        **grant(16, 5 * 10**9),
    )(in_hbm(hop_two))
    prep = pl.pallas_call(
        functools.partial(prep_kernel, feat),
        out_shape=[
            pltpu.VMEM((hidden, 2 * feats), BF16),
            pltpu.VMEM((2, outs, hidden), BF16),
            pltpu.VMEM((feats, seed_dev), BF16),
            pltpu.VMEM((hidden, 128), F32),
            pltpu.VMEM((outs, 128), F32),
        ],
        in_specs=[vmem] * (2 + feat),
        out_specs=[vmem] * 5,
        name="prep_kernel",
        **grant(8, 10**9),
    )
    ready = prep(*map(in_hbm, (w1_self, w1_neigh)), *pieces)
    return pl.pallas_call(
        functools.partial(layer_kernel, fan_two),
        out_shape=jax.ShapeDtypeStruct((outs // feat, seed_dev), F32),
        in_specs=[smem] + [vmem] * 8 + [hbm],
        out_specs=vmem,
        scratch_shapes=[
            pltpu.VMEM((feats, slots), BF16),
            staging,
            pltpu.SemaphoreType.DMA((late,)),
            pltpu.VMEM((fan_one + 1, 2 * feats, seed_dev), BF16),
            pltpu.VMEM((feats, seed_dev), F32),
            pltpu.VMEM((outs, seed_dev), F32),
        ],
        name="layer_kernel",
        **grant(24, 5 * 10**9),
    )(live_counts, fetched, hop_one, *ready, held_counts, in_hbm(late_counts))


def solution(mesh):
    return jax.shard_map(
        per_device,
        mesh=mesh,
        in_specs=(
            P("feat", "dom"),
            P("dom"),
            P("dom", None, None),
            P("dom", None),
            P(None, "dom"),
            P(None, None, "dom"),
            P(),
            P(),
            P("feat"),
            P(None, "feat"),
            P(None, "feat"),
            P("feat"),
        ),
        out_specs=P("feat", "dom"),
        check_vma=False,
    )
```

```python
import functools

import jax
import jax.numpy as jnp
from jax import lax
from jax.experimental import pallas as pl
from jax.experimental.pallas import tpu as pltpu
from jax.sharding import PartitionSpec as P


BF16 = jnp.bfloat16
F32 = jnp.float32
LANES = 256
PARTS = 3
HELD_BYTES = 1 << 21
TILE = 32
LOADS = 4
SMALLS = 5
COUNT = jnp.float8_e4m3fn


def from_where(me, k, feat):
    if feat & (feat - 1) == 0:
        return me ^ k
    return (me - k) % feat


def in_hbm(x):
    return pltpu.with_memory_space_constraint(x, pltpu.HBM)


def grant(mib, flops):
    return dict(
        compiler_params=pltpu.CompilerParams(vmem_limit_bytes=mib << 20),
        cost_estimate=pl.CostEstimate(flops=flops, bytes_accessed=1 << 20, transcendentals=0),
    )


def pick_columns(feats_ref, rows, emit, ready=None):
    feat_dev, nodes = feats_ref.shape
    group = max(1, min(256 // feat_dev, nodes // LANES))
    for start in range(0, rows.shape[1], LANES):
        want = rows[:, start : start + LANES]
        width = want.shape[1]
        high = want >> 8
        low = want & (LANES - 1)
        place = lax.broadcasted_iota(jnp.int32, (LANES, width), 0)
        pick = jnp.where(low == place, 1.0, 0.0).astype(BF16)
        total = jnp.zeros((feat_dev, width), F32)
        for first in range(0, nodes // LANES, group):
            if ready is not None and start == 0:
                ready(first * LANES)
            left = jnp.concatenate(
                [
                    feats_ref[:, (first + i) * LANES : (first + i + 1) * LANES]
                    for i in range(group)
                ],
                axis=0,
            )
            part = jnp.dot(left, pick, preferred_element_type=F32)
            for i in range(group):
                total = jnp.where(
                    high == first + i, part[i * feat_dev : (i + 1) * feat_dev], total
                )
        emit(start, total)


def early_kernel(feats_ref, *rest):
    sources, (out_ref, near_ref, sems), scratch = rest[:SMALLS], rest[SMALLS : SMALLS + 3], rest[-SMALLS:]
    rows_ref, w2s_ref, w2n_ref, b1_ref, b2_ref = scratch
    hid_dev, outs = w2s_ref.shape
    feat_dev, nodes = feats_ref.shape
    loads = LOADS
    width = nodes // loads
    smalls = [
        pltpu.make_async_copy(source, scratch[i], sems.at[loads + i])
        for i, source in enumerate(sources)
    ]

    def load(i):
        part = (slice(None), pl.ds(i * width, width))
        return pltpu.make_async_copy(feats_ref.at[part], near_ref.at[part], sems.at[i])

    for copy in smalls:
        copy.start()
    for i in range(loads):
        load(i).start()
    for copy in smalls:
        copy.wait()
    out_ref[0:outs, 0:hid_dev] = w2s_ref[...].astype(F32).T.astype(BF16)
    out_ref[0:outs, hid_dev : 2 * hid_dev] = w2n_ref[...].astype(F32).T.astype(BF16)
    base = outs + (rows_ref.shape[1] // 128) * feat_dev
    for at, bias_ref in ((0, b1_ref), (hid_dev, b2_ref)):
        left = jnp.broadcast_to(bias_ref[...], (16, hid_dev))
        line = lax.broadcasted_iota(jnp.int32, left.shape, 0)
        parts = jnp.zeros_like(left)
        for i in range(PARTS):
            piece = left.astype(BF16).astype(F32)
            left = left - piece
            parts = jnp.where(line == i, piece, parts)
        out_ref[base : base + 16, at : at + hid_dev] = parts.astype(BF16)

    def emit(start, value):
        for i in range(value.shape[1] // 128):
            at = outs + (start // 128 + i) * feat_dev
            out_ref[at : at + feat_dev, :] = value[:, i * 128 : (i + 1) * 128].astype(BF16)

    def ready(column):
        if column % width == 0:
            load(column // width).wait()

    pick_columns(near_ref, rows_ref[...], emit, ready)


def fetch_kernel(feat, feats_ref, rows_ref, out_ref):
    def emit(start, value):
        for i in range(value.shape[1] // 128):
            piece = value[:, i * 128 : (i + 1) * 128].astype(BF16)
            for copy in range(feat):
                out_ref[(start // 128 + i) * feat + copy] = piece

    pick_columns(feats_ref, rows_ref[...], emit)


def multiplicities(two_ref, times):
    fan_two, fan_one, seeds = two_ref.shape
    for sample in range(fan_two):
        total = jnp.zeros((fan_one, seeds), F32)
        for other in range(fan_two):
            total = total + jnp.where(two_ref[sample] == two_ref[other], 1.0, 0.0)
        times[sample] = total


def make_counts(first, count, two_ref, times, made, out_ref=None, sems=None):
    seeds = two_ref.shape[2]
    fan_two = two_ref.shape[0]
    slots = made.shape[1]
    shape = (TILE, 128)
    i8 = jnp.int8
    line = lax.broadcasted_iota(jnp.int32, shape, 0)
    places = [(line + TILE * i).astype(i8) for i in range(128 // TILE)]
    none = jnp.full(shape, -1, i8)

    def step(j, carry):
        at_j = pl.ds(first + j, 1)
        rows = [two_ref[k, at_j, :] for k in range(fan_two)]
        weights = [times[k, at_j, :] for k in range(fan_two)]
        for at in range(0, seeds, 128):
            wide = [jnp.broadcast_to(row[:, at : at + 128], shape) for row in rows]
            low = [(value & 127).astype(i8) for value in wide]
            high = [(value >> 7).astype(i8) for value in wide]
            times_of = [
                jnp.broadcast_to(row[:, at : at + 128], shape).astype(COUNT) for row in weights
            ]
            for block in range(slots // 128):
                here = jnp.full(shape, block, i8)
                value = [jnp.where(h == here, v, none) for h, v in zip(high, low)]
                for i, place in enumerate(places):
                    total = jnp.zeros(shape, COUNT)
                    for k in range(fan_two):
                        total = jnp.where(value[k] == place, times_of[k], total)
                    start = block * 128 + i * TILE
                    made[j, start : start + TILE, at : at + 128] = total
        if out_ref is not None:
            pltpu.make_async_copy(made.at[j], out_ref.at[j], sems.at[j]).start()
        return carry

    lax.fori_loop(0, count, step, 0)


def late_kernel(held, two_ref, held_ref, out_ref, times, made, sems):
    late = out_ref.shape[0]
    multiplicities(two_ref, times)
    make_counts(held, late, two_ref, times, made, out_ref, sems)
    make_counts(0, held, two_ref, times, held_ref)
    for j in range(late):
        pltpu.make_async_copy(made.at[j], out_ref.at[j], sems.at[j]).wait()


def prep_kernel(feat, w1s_ref, w1n_ref, *rest):
    pieces = rest[:feat]
    w1, w2, x_seed, bias_one, bias_out = rest[feat:]
    hidden, feats = w1s_ref.shape
    outs = w2.shape[1]
    hid_dev = hidden // feat
    feat_dev = feats // feat
    seeds = x_seed.shape[1]
    me = lax.axis_index("feat")
    bias_base = outs + (seeds // 128) * feat_dev
    for k in range(feat):
        owner = from_where(me, k, feat)
        rows = pl.ds(pl.multiple_of(owner * hid_dev, hid_dev), hid_dev)
        here = slice(k * hid_dev, (k + 1) * hid_dev)
        w1[here, 0:feats] = w1s_ref[rows, :]
        w1[here, feats : 2 * feats] = w1n_ref[rows, :]
        at = pl.multiple_of(owner * feat_dev, feat_dev)
        for i in range(seeds // 128):
            first = outs + i * feat_dev
            x_seed[pl.ds(at, feat_dev), i * 128 : (i + 1) * 128] = pieces[k][
                first : first + feat_dev, 0:128
            ]
        parts = pieces[k][bias_base : bias_base + 16, :].astype(F32)
        bias = parts[0:1] + parts[1:2] + parts[2:3]
        column = jnp.broadcast_to(bias, (8, 128)).T
        bias_one[here, :] = jnp.broadcast_to(column[0:hid_dev, 0:1], (hid_dev, 128))
        bias_out[rows, :] = jnp.broadcast_to(column[hid_dev : 2 * hid_dev, 0:1], (hid_dev, 128))
    for index in range(2):
        w2[index] = jnp.concatenate(
            [
                pieces[k][0:outs, :][:, index * hid_dev : (index + 1) * hid_dev]
                for k in range(feat)
            ],
            axis=1,
        )


def add_bias(value, bias_ref):
    return value + jnp.concatenate([bias_ref[...]] * (value.shape[1] // 128), axis=1)


def layer_kernel(
    fan_two, live_ref, fetched_ref, one_ref, w1, w2, x_seed, bias_one, bias_out, held_ref, late_ref, *rest
):
    out_ref, table, staging, sems, both, x_sum, g_sum = rest
    owners, feats, cap = fetched_ref.shape
    fan_one, seeds = one_ref.shape
    held, late = held_ref.shape[0], late_ref.shape[0]
    outs = w2.shape[1]
    me = lax.axis_index("feat")

    def late_copy(j):
        return pltpu.make_async_copy(late_ref.at[j], staging.at[j], sems.at[j])

    for j in range(late):
        late_copy(j).start()
    slot = lax.broadcasted_iota(jnp.int32, (feats, cap), 1)
    for owner in range(owners):
        value = fetched_ref[owner].astype(F32)
        value = jnp.where(slot < live_ref[0, owner], value, 0.0)
        table[:, owner * cap : (owner + 1) * cap] = value.astype(BF16)
    x_sum[...] = jnp.zeros_like(x_sum)

    def aggregate(j, counts):
        place = lax.broadcasted_iota(jnp.int32, (owners * cap, seeds), 0)
        pick = jnp.where(one_ref[j : j + 1, :] == place, 1.0, 0.0).astype(BF16)
        own = jnp.dot(table[...], pick, preferred_element_type=F32)
        mean = jnp.dot(table[...], counts, preferred_element_type=F32)
        x_sum[...] += own
        both[j, 0:feats] = own.astype(BF16)
        both[j, feats : 2 * feats] = (mean * (1.0 / fan_two)).astype(BF16)

    for j in range(held - 1):
        aggregate(j, held_ref[j])
    for j in range(late):
        late_copy(j).wait()
    aggregate(held - 1, held_ref[held - 1])
    for j in range(late):
        aggregate(held + j, staging[j])
    both[fan_one, 0:feats] = x_seed[...]
    both[fan_one, feats : 2 * feats] = (x_sum[...] * (1.0 / fan_one)).astype(BF16)

    def layer(j):
        pre = jnp.dot(w1[...], both[j], preferred_element_type=F32)
        return jnp.maximum(add_bias(pre, bias_one), 0.0)

    total = layer(0)
    for j in range(1, fan_one):
        total = total + layer(j)
    g_sum[...] = total

    z = add_bias(jnp.zeros((outs, seeds), F32), bias_out)
    for index, value in enumerate((layer(fan_one), g_sum[...] * (1.0 / fan_one))):
        high = value.astype(BF16)
        low = (value - high.astype(F32)).astype(BF16)
        z = z + jnp.dot(w2[index], high, preferred_element_type=F32)
        z = z + jnp.dot(w2[index], low, preferred_element_type=F32)
    square = jnp.sum(z * z, axis=0, keepdims=True)
    out_dev = out_ref.shape[0]
    g_sum[...] = z * lax.rsqrt(square * (1.0 / outs) + 1.0)
    out_ref[...] = g_sum[pl.ds(pl.multiple_of(me * out_dev, out_dev), out_dev), :]


def per_device(
    features,
    seed_rows,
    want_rows,
    live_counts,
    hop_one,
    hop_two,
    w1_self,
    w1_neigh,
    b1,
    w2_self,
    w2_neigh,
    b2,
):
    feat_dev = features.shape[0]
    seed_dev = seed_rows.shape[0]
    owners, cap = want_rows.shape[1:]
    feat = lax.axis_size("feat")
    feats = feat * feat_dev
    outs, hidden = w1_self.shape[0], w1_self.shape[0]
    slots = owners * cap
    fan_two, fan_one = hop_two.shape[:2]
    vmem = pl.BlockSpec(memory_space=pltpu.VMEM)
    hbm = pl.BlockSpec(memory_space=pltpu.HBM)
    smem = pl.BlockSpec(memory_space=pltpu.SMEM)

    asked = lax.all_to_all(want_rows, "dom", split_axis=1, concat_axis=0, tiled=True)
    rows = outs + (seed_dev // 128) * feat_dev + 16
    held = max(1, min(fan_one - 1, HELD_BYTES // (slots * seed_dev)))
    late = fan_one - held
    two_vmem = pltpu.VMEM(hop_two.shape, F32)
    smalls = (seed_rows[None], w2_self.T, w2_neigh.T, b1[None], b2[None])
    mine, near = pl.pallas_call(
        early_kernel,
        out_shape=[pltpu.VMEM((rows, 128), BF16), pltpu.VMEM(features.shape, BF16)],
        in_specs=[hbm] * (1 + SMALLS),
        out_specs=[vmem] * 2,
        scratch_shapes=[pltpu.SemaphoreType.DMA((LOADS + SMALLS,))]
        + [pltpu.VMEM(x.shape, x.dtype) for x in smalls],
        name="early_kernel",
        **grant(8, 10**9),
    )(*map(in_hbm, (features,) + smalls))
    pieces = [mine]
    for k in range(1, feat):
        pairs = [(from_where(i, k, feat), i) for i in range(feat)]
        pieces.append(lax.ppermute(mine, "feat", pairs))
    fetch = pl.pallas_call(
        functools.partial(fetch_kernel, feat),
        out_shape=pltpu.VMEM((owners * feat, feat_dev, cap), BF16),
        in_specs=[vmem] * 2,
        out_specs=vmem,
        name="fetch_kernel",
        **grant(8, 10**9),
    )
    served = fetch(near, asked.reshape(1, slots))
    fetched = lax.all_to_all(
        served, ("dom", "feat"), split_axis=0, concat_axis=0, tiled=True
    )
    fetched = fetched.reshape(owners, feats, cap)
    block = (slots, seed_dev)
    staging = pltpu.VMEM((late,) + block, COUNT)
    held_counts, late_counts = pl.pallas_call(
        functools.partial(late_kernel, held),
        out_shape=[pltpu.VMEM((held,) + block, COUNT), pltpu.HBM((late,) + block, COUNT)],
        in_specs=[vmem],
        out_specs=[vmem, hbm],
        scratch_shapes=[two_vmem, staging, pltpu.SemaphoreType.DMA((late,))],
        name="late_kernel",
        **grant(16, 5 * 10**9),
    )(in_hbm(hop_two))
    prep = pl.pallas_call(
        functools.partial(prep_kernel, feat),
        out_shape=[
            pltpu.VMEM((hidden, 2 * feats), BF16),
            pltpu.VMEM((2, outs, hidden), BF16),
            pltpu.VMEM((feats, seed_dev), BF16),
            pltpu.VMEM((hidden, 128), F32),
            pltpu.VMEM((outs, 128), F32),
        ],
        in_specs=[vmem] * (2 + feat),
        out_specs=[vmem] * 5,
        name="prep_kernel",
        **grant(8, 10**9),
    )
    ready = prep(*map(in_hbm, (w1_self, w1_neigh)), *pieces)
    return pl.pallas_call(
        functools.partial(layer_kernel, fan_two),
        out_shape=jax.ShapeDtypeStruct((outs // feat, seed_dev), F32),
        in_specs=[smem] + [vmem] * 8 + [hbm],
        out_specs=vmem,
        scratch_shapes=[
            pltpu.VMEM((feats, slots), BF16),
            staging,
            pltpu.SemaphoreType.DMA((late,)),
            pltpu.VMEM((fan_one + 1, 2 * feats, seed_dev), BF16),
            pltpu.VMEM((feats, seed_dev), F32),
            pltpu.VMEM((outs, seed_dev), F32),
        ],
        name="layer_kernel",
        **grant(24, 5 * 10**9),
    )(live_counts, fetched, hop_one, *ready, held_counts, in_hbm(late_counts))


def solution(mesh):
    return jax.shard_map(
        per_device,
        mesh=mesh,
        in_specs=(
            P("feat", "dom"),
            P("dom"),
            P("dom", None, None),
            P("dom", None),
            P(None, "dom"),
            P(None, None, "dom"),
            P(),
            P(),
            P("feat"),
            P(None, "feat"),
            P(None, "feat"),
            P("feat"),
        ),
        out_specs=P("feat", "dom"),
        check_vma=False,
    )
```

```python
import functools

import jax
import jax.numpy as jnp
from jax import lax
from jax.experimental import pallas as pl
from jax.experimental.pallas import tpu as pltpu
from jax.sharding import PartitionSpec as P


BF16 = jnp.bfloat16
F32 = jnp.float32
LANES = 256
PARTS = 3
HELD_BYTES = 1 << 21
TILE = 32
LOADS = 4
SMALLS = 5
COUNT = jnp.float8_e4m3fn


def from_where(me, k, feat):
    if feat & (feat - 1) == 0:
        return me ^ k
    return (me - k) % feat


def in_hbm(x):
    return pltpu.with_memory_space_constraint(x, pltpu.HBM)


def grant(mib, flops):
    return dict(
        compiler_params=pltpu.CompilerParams(vmem_limit_bytes=mib << 20),
        cost_estimate=pl.CostEstimate(flops=flops, bytes_accessed=1 << 20, transcendentals=0),
    )


def pick_columns(feats_ref, rows, emit, ready=None):
    feat_dev, nodes = feats_ref.shape
    group = max(1, min(128 // feat_dev, nodes // LANES))
    for start in range(0, rows.shape[1], 2 * LANES):
        want = rows[:, start : start + 2 * LANES]
        width = want.shape[1]
        high = want >> 8
        low = want & (LANES - 1)
        place = lax.broadcasted_iota(jnp.int32, (LANES, width), 0)
        pick = jnp.where(low == place, 1.0, 0.0).astype(BF16)
        total = jnp.zeros((feat_dev, width), F32)
        for first in range(0, nodes // LANES, group):
            if ready is not None and start == 0:
                ready(first * LANES)
            left = jnp.concatenate(
                [
                    feats_ref[:, (first + i) * LANES : (first + i + 1) * LANES]
                    for i in range(group)
                ],
                axis=0,
            )
            part = jnp.dot(left, pick, preferred_element_type=F32)
            for i in range(group):
                total = jnp.where(
                    high == first + i, part[i * feat_dev : (i + 1) * feat_dev], total
                )
        emit(start, total)


def early_kernel(feats_ref, *rest):
    sources, (out_ref, near_ref, sems), scratch = rest[:SMALLS], rest[SMALLS : SMALLS + 3], rest[-SMALLS:]
    rows_ref, w2s_ref, w2n_ref, b1_ref, b2_ref = scratch
    hid_dev, outs = w2s_ref.shape
    feat_dev, nodes = feats_ref.shape
    loads = LOADS
    width = nodes // loads
    smalls = [
        pltpu.make_async_copy(source, scratch[i], sems.at[loads + i])
        for i, source in enumerate(sources)
    ]

    def load(i):
        part = (slice(None), pl.ds(i * width, width))
        return pltpu.make_async_copy(feats_ref.at[part], near_ref.at[part], sems.at[i])

    for copy in smalls:
        copy.start()
    for i in range(loads):
        load(i).start()
    for copy in smalls:
        copy.wait()
    out_ref[0:outs, 0:hid_dev] = w2s_ref[...].astype(F32).T.astype(BF16)
    out_ref[0:outs, hid_dev : 2 * hid_dev] = w2n_ref[...].astype(F32).T.astype(BF16)
    base = outs + (rows_ref.shape[1] // 128) * feat_dev
    for at, bias_ref in ((0, b1_ref), (hid_dev, b2_ref)):
        left = jnp.broadcast_to(bias_ref[...], (16, hid_dev))
        line = lax.broadcasted_iota(jnp.int32, left.shape, 0)
        parts = jnp.zeros_like(left)
        for i in range(PARTS):
            piece = left.astype(BF16).astype(F32)
            left = left - piece
            parts = jnp.where(line == i, piece, parts)
        out_ref[base : base + 16, at : at + hid_dev] = parts.astype(BF16)

    def emit(start, value):
        for i in range(value.shape[1] // 128):
            at = outs + (start // 128 + i) * feat_dev
            out_ref[at : at + feat_dev, :] = value[:, i * 128 : (i + 1) * 128].astype(BF16)

    def ready(column):
        if column % width == 0:
            load(column // width).wait()

    pick_columns(near_ref, rows_ref[...], emit, ready)


def fetch_kernel(feat, feats_ref, rows_ref, out_ref):
    def emit(start, value):
        for i in range(value.shape[1] // 128):
            piece = value[:, i * 128 : (i + 1) * 128].astype(BF16)
            for copy in range(feat):
                out_ref[(start // 128 + i) * feat + copy] = piece

    pick_columns(feats_ref, rows_ref[...], emit)


def multiplicities(two_ref, times):
    fan_two, fan_one, seeds = two_ref.shape
    for sample in range(fan_two):
        total = jnp.zeros((fan_one, seeds), F32)
        for other in range(fan_two):
            total = total + jnp.where(two_ref[sample] == two_ref[other], 1.0, 0.0)
        times[sample] = total


def make_counts(first, count, two_ref, times, made, out_ref=None, sems=None):
    seeds = two_ref.shape[2]
    fan_two = two_ref.shape[0]
    slots = made.shape[1]
    shape = (TILE, 128)
    i8 = jnp.int8
    line = lax.broadcasted_iota(jnp.int32, shape, 0)
    places = [(line + TILE * i).astype(i8) for i in range(128 // TILE)]
    none = jnp.full(shape, -1, i8)

    def step(j, carry):
        at_j = pl.ds(first + j, 1)
        rows = [two_ref[k, at_j, :] for k in range(fan_two)]
        weights = [times[k, at_j, :] for k in range(fan_two)]
        for at in range(0, seeds, 128):
            wide = [jnp.broadcast_to(row[:, at : at + 128], shape) for row in rows]
            low = [(value & 127).astype(i8) for value in wide]
            high = [(value >> 7).astype(i8) for value in wide]
            times_of = [
                jnp.broadcast_to(row[:, at : at + 128], shape).astype(COUNT) for row in weights
            ]
            for block in range(slots // 128):
                here = jnp.full(shape, block, i8)
                value = [jnp.where(h == here, v, none) for h, v in zip(high, low)]
                for i, place in enumerate(places):
                    total = jnp.zeros(shape, COUNT)
                    for k in range(fan_two):
                        total = jnp.where(value[k] == place, times_of[k], total)
                    start = block * 128 + i * TILE
                    made[j, start : start + TILE, at : at + 128] = total
        if out_ref is not None:
            pltpu.make_async_copy(made.at[j], out_ref.at[j], sems.at[j]).start()
        return carry

    lax.fori_loop(0, count, step, 0)


def late_kernel(held, two_ref, held_ref, out_ref, times, made, sems):
    late = out_ref.shape[0]
    multiplicities(two_ref, times)
    make_counts(held, late, two_ref, times, made, out_ref, sems)
    make_counts(0, held, two_ref, times, held_ref)
    for j in range(late):
        pltpu.make_async_copy(made.at[j], out_ref.at[j], sems.at[j]).wait()


def prep_kernel(feat, w1s_ref, w1n_ref, *rest):
    pieces = rest[:feat]
    w1, w2, x_seed, bias_one, bias_out = rest[feat:]
    hidden, feats = w1s_ref.shape
    outs = w2.shape[1]
    hid_dev = hidden // feat
    feat_dev = feats // feat
    seeds = x_seed.shape[1]
    me = lax.axis_index("feat")
    bias_base = outs + (seeds // 128) * feat_dev
    for k in range(feat):
        owner = from_where(me, k, feat)
        rows = pl.ds(pl.multiple_of(owner * hid_dev, hid_dev), hid_dev)
        here = slice(k * hid_dev, (k + 1) * hid_dev)
        w1[here, 0:feats] = w1s_ref[rows, :]
        w1[here, feats : 2 * feats] = w1n_ref[rows, :]
        at = pl.multiple_of(owner * feat_dev, feat_dev)
        for i in range(seeds // 128):
            first = outs + i * feat_dev
            x_seed[pl.ds(at, feat_dev), i * 128 : (i + 1) * 128] = pieces[k][
                first : first + feat_dev, 0:128
            ]
        parts = pieces[k][bias_base : bias_base + 16, :].astype(F32)
        bias = parts[0:1] + parts[1:2] + parts[2:3]
        column = jnp.broadcast_to(bias, (8, 128)).T
        bias_one[here, :] = jnp.broadcast_to(column[0:hid_dev, 0:1], (hid_dev, 128))
        bias_out[rows, :] = jnp.broadcast_to(column[hid_dev : 2 * hid_dev, 0:1], (hid_dev, 128))
    for index in range(2):
        w2[index] = jnp.concatenate(
            [
                pieces[k][0:outs, :][:, index * hid_dev : (index + 1) * hid_dev]
                for k in range(feat)
            ],
            axis=1,
        )


def add_bias(value, bias_ref):
    return value + jnp.concatenate([bias_ref[...]] * (value.shape[1] // 128), axis=1)


def layer_kernel(
    fan_two, live_ref, fetched_ref, one_ref, w1, w2, x_seed, bias_one, bias_out, held_ref, late_ref, *rest
):
    out_ref, table, staging, sems, both, x_sum, g_sum = rest
    owners, feats, cap = fetched_ref.shape
    fan_one, seeds = one_ref.shape
    held, late = held_ref.shape[0], late_ref.shape[0]
    outs = w2.shape[1]
    me = lax.axis_index("feat")

    def late_copy(j):
        return pltpu.make_async_copy(late_ref.at[j], staging.at[j], sems.at[j])

    for j in range(late):
        late_copy(j).start()
    slot = lax.broadcasted_iota(jnp.int32, (feats, cap), 1)
    for owner in range(owners):
        value = fetched_ref[owner].astype(F32)
        value = jnp.where(slot < live_ref[0, owner], value, 0.0)
        table[:, owner * cap : (owner + 1) * cap] = value.astype(BF16)
    x_sum[...] = jnp.zeros_like(x_sum)

    def aggregate(j, counts):
        place = lax.broadcasted_iota(jnp.int32, (owners * cap, seeds), 0)
        pick = jnp.where(one_ref[j : j + 1, :] == place, 1.0, 0.0).astype(BF16)
        own = jnp.dot(table[...], pick, preferred_element_type=F32)
        mean = jnp.dot(table[...], counts, preferred_element_type=F32)
        x_sum[...] += own
        both[j, 0:feats] = own.astype(BF16)
        both[j, feats : 2 * feats] = (mean * (1.0 / fan_two)).astype(BF16)

    for j in range(held - 1):
        aggregate(j, held_ref[j])
    for j in range(late):
        late_copy(j).wait()
    aggregate(held - 1, held_ref[held - 1])
    for j in range(late):
        aggregate(held + j, staging[j])
    both[fan_one, 0:feats] = x_seed[...]
    both[fan_one, feats : 2 * feats] = (x_sum[...] * (1.0 / fan_one)).astype(BF16)

    def layer(j):
        pre = jnp.dot(w1[...], both[j], preferred_element_type=F32)
        return jnp.maximum(add_bias(pre, bias_one), 0.0)

    total = layer(0)
    for j in range(1, fan_one):
        total = total + layer(j)
    g_sum[...] = total

    z = add_bias(jnp.zeros((outs, seeds), F32), bias_out)
    for index, value in enumerate((layer(fan_one), g_sum[...] * (1.0 / fan_one))):
        high = value.astype(BF16)
        low = (value - high.astype(F32)).astype(BF16)
        z = z + jnp.dot(w2[index], high, preferred_element_type=F32)
        z = z + jnp.dot(w2[index], low, preferred_element_type=F32)
    square = jnp.sum(z * z, axis=0, keepdims=True)
    out_dev = out_ref.shape[0]
    g_sum[...] = z * lax.rsqrt(square * (1.0 / outs) + 1.0)
    out_ref[...] = g_sum[pl.ds(pl.multiple_of(me * out_dev, out_dev), out_dev), :]


def per_device(
    features,
    seed_rows,
    want_rows,
    live_counts,
    hop_one,
    hop_two,
    w1_self,
    w1_neigh,
    b1,
    w2_self,
    w2_neigh,
    b2,
):
    feat_dev = features.shape[0]
    seed_dev = seed_rows.shape[0]
    owners, cap = want_rows.shape[1:]
    feat = lax.axis_size("feat")
    feats = feat * feat_dev
    outs, hidden = w1_self.shape[0], w1_self.shape[0]
    slots = owners * cap
    fan_two, fan_one = hop_two.shape[:2]
    vmem = pl.BlockSpec(memory_space=pltpu.VMEM)
    hbm = pl.BlockSpec(memory_space=pltpu.HBM)
    smem = pl.BlockSpec(memory_space=pltpu.SMEM)

    asked = lax.all_to_all(want_rows, "dom", split_axis=1, concat_axis=0, tiled=True)
    rows = outs + (seed_dev // 128) * feat_dev + 16
    held = max(1, min(fan_one - 1, HELD_BYTES // (slots * seed_dev)))
    late = fan_one - held
    two_vmem = pltpu.VMEM(hop_two.shape, F32)
    smalls = (seed_rows[None], w2_self.T, w2_neigh.T, b1[None], b2[None])
    mine, near = pl.pallas_call(
        early_kernel,
        out_shape=[pltpu.VMEM((rows, 128), BF16), pltpu.VMEM(features.shape, BF16)],
        in_specs=[hbm] * (1 + SMALLS),
        out_specs=[vmem] * 2,
        scratch_shapes=[pltpu.SemaphoreType.DMA((LOADS + SMALLS,))]
        + [pltpu.VMEM(x.shape, x.dtype) for x in smalls],
        name="early_kernel",
        **grant(8, 10**9),
    )(*map(in_hbm, (features,) + smalls))
    pieces = [mine]
    for k in range(1, feat):
        pairs = [(from_where(i, k, feat), i) for i in range(feat)]
        pieces.append(lax.ppermute(mine, "feat", pairs))
    fetch = pl.pallas_call(
        functools.partial(fetch_kernel, feat),
        out_shape=pltpu.VMEM((owners * feat, feat_dev, cap), BF16),
        in_specs=[vmem] * 2,
        out_specs=vmem,
        name="fetch_kernel",
        **grant(8, 10**9),
    )
    served = fetch(near, asked.reshape(1, slots))
    fetched = lax.all_to_all(
        served, ("dom", "feat"), split_axis=0, concat_axis=0, tiled=True
    )
    fetched = fetched.reshape(owners, feats, cap)
    block = (slots, seed_dev)
    staging = pltpu.VMEM((late,) + block, COUNT)
    held_counts, late_counts = pl.pallas_call(
        functools.partial(late_kernel, held),
        out_shape=[pltpu.VMEM((held,) + block, COUNT), pltpu.HBM((late,) + block, COUNT)],
        in_specs=[vmem],
        out_specs=[vmem, hbm],
        scratch_shapes=[two_vmem, staging, pltpu.SemaphoreType.DMA((late,))],
        name="late_kernel",
        **grant(16, 5 * 10**9),
    )(in_hbm(hop_two))
    prep = pl.pallas_call(
        functools.partial(prep_kernel, feat),
        out_shape=[
            pltpu.VMEM((hidden, 2 * feats), BF16),
            pltpu.VMEM((2, outs, hidden), BF16),
            pltpu.VMEM((feats, seed_dev), BF16),
            pltpu.VMEM((hidden, 128), F32),
            pltpu.VMEM((outs, 128), F32),
        ],
        in_specs=[vmem] * (2 + feat),
        out_specs=[vmem] * 5,
        name="prep_kernel",
        **grant(8, 10**9),
    )
    ready = prep(*map(in_hbm, (w1_self, w1_neigh)), *pieces)
    return pl.pallas_call(
        functools.partial(layer_kernel, fan_two),
        out_shape=jax.ShapeDtypeStruct((outs // feat, seed_dev), F32),
        in_specs=[smem] + [vmem] * 8 + [hbm],
        out_specs=vmem,
        scratch_shapes=[
            pltpu.VMEM((feats, slots), BF16),
            staging,
            pltpu.SemaphoreType.DMA((late,)),
            pltpu.VMEM((fan_one + 1, 2 * feats, seed_dev), BF16),
            pltpu.VMEM((feats, seed_dev), F32),
            pltpu.VMEM((outs, seed_dev), F32),
        ],
        name="layer_kernel",
        **grant(24, 5 * 10**9),
    )(live_counts, fetched, hop_one, *ready, held_counts, in_hbm(late_counts))


def solution(mesh):
    return jax.shard_map(
        per_device,
        mesh=mesh,
        in_specs=(
            P("feat", "dom"),
            P("dom"),
            P("dom", None, None),
            P("dom", None),
            P(None, "dom"),
            P(None, None, "dom"),
            P(),
            P(),
            P("feat"),
            P(None, "feat"),
            P(None, "feat"),
            P("feat"),
        ),
        out_specs=P("feat", "dom"),
        check_vma=False,
    )
```
